32 devices in a mesh: lat: 8 (over z, x), lev: 4 (over y, core).
Axes of the slice: x: 2, y: 2, z: 4, core: 2. Of those that a mesh axis runs over, the one named last changes fastest.
Arguments:
- grid: bfloat16 [640, 128, 4, 1280], P('lat', 'lev'), may hold values from -6 to 6
- legendre: bfloat16 [640, 640, 640], P('lat'), may hold values from -0.25 to 0.25
- vertical: bfloat16 [128, 128], P('lev'), may hold values from -0.5 to 0.5
- damping: bfloat16 [128], P('lev'), may hold values from 1 to 16
- lon_counts: int32 [640], replicated, may hold values from 160 to 1280
- wave_slots: int32 [640], replicated, may hold values from 0 to 639, as said below
Outputs:
- filtered_grid: bfloat16 [640, 128, 4, 1280], P('lat', 'lev')
The draws below stay inside these ranges and needn't reach their ends.
Inputs may be any that keep to these rules, and one draw needn't show every extreme that they name: wave_slots is a permutation; slot g * 20 + r holds a wavenumber from r * 32 to (r + 1) * 32 - 1.
All inputs are finite; a program needn't handle non-finite values.
Results may differ from the reference program's by a relative error of at most 0.0074.
Values may be sent and summed in bfloat16 or wider, within the bound.
A program may use at most 512 MiB of HBM per device.

```python
import math
import jax
import jax.numpy as jnp
from jax import lax

NLAT = 640
NLON = 1280
M = 640
FIELDS = 4
LEV = 128
GROUPS = 32
ROUNDS = 20


def draw_wave_slots(key, part):
    keys = jax.random.split(jax.random.fold_in(key, 11), ROUNDS)
    orders = jax.vmap(lambda single: jax.random.permutation(single, GROUPS))(keys)
    base = jnp.arange(ROUNDS, dtype=jnp.int32)[:, None] * GROUPS
    return (base + orders.astype(jnp.int32)).T.reshape(M).astype(jnp.int32)


def place_ends(drawn, rng, smallest, top_value):
    index_at = [jax.random.randint(jax.random.fold_in(rng, axis), (), 0, length) for axis, length in enumerate(drawn.shape)]
    main_axis = drawn.shape.index(max(drawn.shape))
    neighbour = index_at[:main_axis] + [(index_at[main_axis] + 1) % drawn.shape[main_axis]] + index_at[main_axis + 1:]
    return drawn.at[tuple(index_at)].set(smallest).at[tuple(neighbour)].set(top_value)


def block_levels(key, dims, cuts, least, largest):
    def one(dim, blocks):
        steps = jax.random.uniform(jax.random.fold_in(jax.random.fold_in(key, 6), dim), (blocks,), jnp.float32, least / len(cuts), largest / len(cuts))
        return jnp.repeat(jnp.exp(steps), dims[dim] // blocks).reshape((-1,) + (1,) * (len(dims) - dim - 1))

    loudness = one(*cuts[0])
    for cut in cuts[1:]:
        loudness = loudness * one(*cut)
    return loudness


def centred(rng, extent, scale, bound, pieces=(), kind=jnp.bfloat16):
    result = scale * jax.random.normal(rng, extent, jnp.float32)
    if pieces:
        result = result * block_levels(rng, extent, pieces, -0.22, 0.18)
    return jnp.clip(result, -bound, bound).astype(kind)


def setup_inputs(seed: int = 0) -> dict:
    splits = jax.random.split(jax.random.key(seed), 7)
    return {
        "grid": centred(splits[0], (NLAT, LEV, FIELDS, NLON), 1.0, 6.0, ((0, 8), (1, 4))),
        "legendre": centred(splits[1], (M, M, NLAT), NLAT ** -0.5, 0.25, ((0, 8),)),
        "vertical": centred(splits[2], (LEV, LEV), LEV ** -0.5, 0.5, ((0, 4),)),
        "damping": jnp.clip(jnp.exp(math.log(16.0) - 2.7725887 * jax.random.uniform(splits[3], (LEV,), jnp.float32) ** block_levels(splits[3], (LEV,), ((0, 4),), -0.2, 0.2)), 1.0, 16.0).astype(jnp.bfloat16),
        "lon_counts": place_ends(jax.random.randint(splits[4], (NLAT,), NLON // 8, NLON + 1), jax.random.fold_in(splits[4], 1), NLON // 8, NLON).astype(jnp.int32),
        "wave_slots": draw_wave_slots(jax.random.fold_in(splits[6], 71), 0),
    }


def fourier_tables(wavenumbers, longitudes):
    wavenumbers = wavenumbers.astype(jnp.int32)
    points = jnp.arange(longitudes, dtype=jnp.int32)
    phase = (wavenumbers[:, None] * points[None, :] % longitudes).astype(jnp.float32) * (2.0 * math.pi / longitudes)
    scale = 1.0 / math.sqrt(longitudes)
    cosine = jnp.cos(phase) * scale
    sine = jnp.sin(phase) * scale
    forward_table = jnp.stack([cosine, -sine], axis=1).astype(jnp.bfloat16)
    weight = jnp.where(wavenumbers == 0, 1.0, 2.0).astype(jnp.float32)[:, None]
    inverse_table = jnp.stack([cosine * weight, -sine * weight], axis=1).astype(jnp.bfloat16)
    return (forward_table, inverse_table)

def damping_factor(degrees, damping):
    degree_values = jnp.arange(degrees).astype(jnp.float32)
    ratio = degree_values * (degree_values + 1.0) / float(degrees * (degrees - 1))
    return 1.0 / (1.0 + damping.astype(jnp.float32)[None, :] * (ratio * ratio)[:, None])

def reference(grid, legendre, vertical, damping, lon_counts, wave_slots):
    latitudes, levels, fields, longitudes = grid.shape
    wavenumbers = wave_slots.astype(jnp.int32)
    slot_count = wavenumbers.shape[0]
    degrees = legendre.shape[1]
    pair_width = 2 * fields
    forward_table, inverse_table = fourier_tables(wavenumbers, longitudes)
    kept = (2 * wavenumbers[:, None] < lon_counts.astype(jnp.int32)[None, :]).astype(jnp.float32)
    fourier = jnp.einsum('mrx,alfx->mlrfa', forward_table.astype(jnp.float32), grid.astype(jnp.float32))
    fourier = (fourier * kept[:, None, None, None, :]).astype(jnp.bfloat16)
    fourier = fourier.reshape(slot_count, levels * pair_width, latitudes)
    factor = damping_factor(degrees, damping)
    mixer = vertical.astype(jnp.float32)

    def one_slot(item):
        table, block, wave = item
        spectral = jnp.dot(table, block.T, preferred_element_type=jnp.float32)
        live = (jnp.arange(degrees, dtype=jnp.int32) >= wave).astype(jnp.float32)
        spectral = (spectral * live[:, None]).astype(jnp.bfloat16).reshape(degrees, levels, pair_width)
        stacked = spectral.astype(jnp.float32)
        mixed = (stacked + jnp.einsum('nkc,lk->nlc', stacked, mixer)) * factor[:, :, None]
        mixed = mixed.astype(jnp.bfloat16).reshape(degrees, levels * pair_width)
        banded = jnp.dot(mixed.T, table, preferred_element_type=jnp.float32)
        return banded.astype(jnp.bfloat16)
    banded = lax.map(one_slot, (legendre, fourier, wavenumbers))
    banded = banded.reshape(slot_count, levels, 2, fields, latitudes).astype(jnp.float32) * kept[:, None, None, None, :]
    filtered_grid = jnp.einsum('mlrfa,mrx->alfx', banded, inverse_table.astype(jnp.float32))
    return filtered_grid.astype(jnp.bfloat16)
```

```python
import functools
import math

import jax
import jax.numpy as jnp
from jax import lax
from jax.experimental import pallas as pl
from jax.experimental.pallas import tpu as pltpu
from jax.sharding import PartitionSpec as P

CHUNKS = 4
VMEM_LIMIT = 60 * 1024 * 1024


def table_build(wavenumbers, longitudes):
    points = jnp.arange(longitudes, dtype=jnp.int32)
    phase = (wavenumbers[:, None] * points[None, :] % longitudes).astype(jnp.float32) * (
        2.0 * math.pi / longitudes
    )
    scale = 1.0 / math.sqrt(longitudes)
    return jnp.concatenate([jnp.cos(phase) * scale, -jnp.sin(phase) * scale], axis=0).astype(
        jnp.bfloat16
    )


def row_block(rows):
    return 16 if rows % 16 == 0 else rows


def forward_body(block, padded, cols, lon_ref, grid_ref, table_ref, wave_ref, out_ref, held):
    base = pl.program_id(0) * block
    both = table_ref.shape[0]
    step = 2 if block % 2 == 0 else 1
    for row in range(0, block, step):
        points = grid_ref[row : row + step].reshape(step * cols, grid_ref.shape[2])
        result = lax.dot_general(
            table_ref[...], points, (((1,), (1,)), ((), ())), preferred_element_type=jnp.float32
        )
        for part in range(step):
            keep = 2 * wave_ref[...] < lon_ref[base + row + part]
            piece = result[:, part * cols : (part + 1) * cols]
            held[pl.ds(row + part, both, stride=padded), :] = jnp.where(keep, piece, 0.0)
    half = both // 2
    full = held[...].reshape(2, half, padded, cols)
    for part in range(2):
        out_ref[:, part] = full[part, :, :block].astype(out_ref.dtype)


def forward_fourier(grid, table, waves, counts):
    rows, cols, longitudes = grid.shape
    both = table.shape[0]
    block = row_block(rows)
    padded = -(-block // 8) * 8
    return pl.pallas_call(
        functools.partial(forward_body, block, padded, cols),
        out_shape=jax.ShapeDtypeStruct((both // 2, 2, rows, cols), jnp.bfloat16),
        grid_spec=pltpu.PrefetchScalarGridSpec(
            num_scalar_prefetch=1,
            grid=(rows // block,),
            in_specs=[
                pl.BlockSpec((block, cols, longitudes), lambda i, c: (i, 0, 0)),
                pl.BlockSpec((both, longitudes), lambda i, c: (0, 0)),
                pl.BlockSpec((both, cols), lambda i, c: (0, 0)),
            ],
            out_specs=pl.BlockSpec((both // 2, 2, block, cols), lambda i, c: (0, 0, i, 0)),
            scratch_shapes=[pltpu.VMEM((both * padded, cols), jnp.float32)],
        ),
        compiler_params=pltpu.CompilerParams(vmem_limit_bytes=VMEM_LIMIT),
        cost_estimate=pl.CostEstimate(
            flops=2 * both * rows * cols * longitudes,
            bytes_accessed=2 * rows * cols * (longitudes + both),
            transcendentals=0,
        ),
        name="forward_fourier",
    )(counts, grid, table, waves)


def spectral_body(lat_size, lev_size, rows, cols, own_ref, wave_ref, table_ref, in_ref, mixer_ref, factor_ref, out_ref):
    table = table_ref[0]
    degrees = table.shape[0]
    width = lev_size * cols
    wave = wave_ref[pl.program_id(0)]
    live = lax.broadcasted_iota(jnp.int32, (degrees, width), 0) >= wave
    for part in range(2):
        fourier = jnp.concatenate(
            [
                jnp.concatenate(
                    [in_ref[i * lev_size + j, 0, part] for i in range(lat_size)], axis=0
                )
                for j in range(lev_size)
            ],
            axis=1,
        )
        spectral = jnp.dot(table, fourier, preferred_element_type=jnp.float32)
        spectral = jnp.where(live, spectral, 0.0).astype(jnp.bfloat16)
        folded = jnp.dot(spectral, mixer_ref[...], preferred_element_type=jnp.float32)
        mixed = ((spectral.astype(jnp.float32) + folded) * factor_ref[...]).astype(jnp.bfloat16)
        banded = lax.dot_general(
            table, mixed, (((0,), (0,)), ((), ())), preferred_element_type=jnp.float32
        ).astype(jnp.bfloat16)
        for i in range(lat_size):
            for j in range(lev_size):
                out_ref[i * lev_size + j, 0, part] = banded[
                    i * rows : (i + 1) * rows, j * cols : (j + 1) * cols
                ]


def spectral_step(legendre, gathered, mixer, factor, first_slot, own_waves, lat_size, lev_size):
    owners, count, _, rows, cols = gathered.shape
    degrees, latitudes = legendre.shape[1:]
    width = lev_size * cols
    block = pl.BlockSpec((owners, 1, 2, rows, cols), lambda s, o, w: (0, s, 0, 0, 0))
    return pl.pallas_call(
        functools.partial(spectral_body, lat_size, lev_size, rows, cols),
        out_shape=jax.ShapeDtypeStruct(gathered.shape, jnp.bfloat16),
        grid_spec=pltpu.PrefetchScalarGridSpec(
            num_scalar_prefetch=2,
            grid=(count,),
            in_specs=[
                pl.BlockSpec((1, degrees, latitudes), lambda s, o, w: (o[0] + s, 0, 0)),
                block,
                pl.BlockSpec((width, width), lambda s, o, w: (0, 0)),
                pl.BlockSpec((degrees, width), lambda s, o, w: (0, 0)),
            ],
            out_specs=block,
        ),
        compiler_params=pltpu.CompilerParams(vmem_limit_bytes=VMEM_LIMIT),
        cost_estimate=pl.CostEstimate(
            flops=count * 4 * degrees * width * (2 * latitudes + width),
            bytes_accessed=2 * count * degrees * latitudes + 4 * gathered.size,
            transcendentals=0,
        ),
        name="spectral_step",
    )(first_slot, own_waves, legendre, gathered, mixer, factor)


def inverse_body(count, block, padded, cols, carried, lon_ref, *refs):
    pieces, tables, waves = refs[:count], refs[count : 2 * count], refs[2 * count : 3 * count]
    before = refs[3 * count] if carried else None
    out_ref = refs[3 * count + (1 if carried else 0)]
    helds = refs[3 * count + (2 if carried else 1) :]
    base = pl.program_id(0) * block
    step = 2 if block % 2 == 0 else 1
    for piece, held in zip(pieces, helds):
        half = piece.shape[0]
        for part in range(2):
            value = piece[:, part].astype(jnp.float32)
            if padded != block:
                value = jnp.pad(value, ((0, 0), (0, padded - block), (0, 0)))
            span = half * padded
            held[part * span : (part + 1) * span, :] = value.reshape(span, cols)
    for row in range(0, block, step):
        total = None
        for held, table, wave in zip(helds, tables, waves):
            both = table.shape[0]
            weight = jnp.where(wave[...] == 0, 1.0, 2.0)
            columns = []
            for part in range(step):
                keep = 2 * wave[...] < lon_ref[base + row + part]
                value = held[pl.ds(row + part, both, stride=padded), :]
                columns.append(jnp.where(keep, value * weight, 0.0).astype(jnp.bfloat16))
            banded = jnp.concatenate(columns, axis=1) if step > 1 else columns[0]
            product = lax.dot_general(
                banded, table[...], (((0,), (0,)), ((), ())), preferred_element_type=jnp.float32
            )
            total = product if total is None else total + product
        total = total.reshape(step, cols, total.shape[1])
        if carried:
            total = total + before[row : row + step]
        out_ref[row : row + step] = total.astype(out_ref.dtype)


def inverse_fourier(pieces, tables, waves, counts, before, kind):
    rows, cols = pieces[0].shape[2:]
    longitudes = tables[0].shape[1]
    block = row_block(rows)
    if block == 16:
        block = 8 if before is None and kind == jnp.float32 or before is not None else 16
    block = 16 if rows % 16 == 0 else rows
    padded = -(-block // 8) * 8
    carried = before is not None
    grid_block = pl.BlockSpec((block, cols, longitudes), lambda i, c: (i, 0, 0))
    in_specs = (
        [pl.BlockSpec((p.shape[0], 2, block, cols), lambda i, c: (0, 0, i, 0)) for p in pieces]
        + [pl.BlockSpec(t.shape, lambda i, c: (0, 0)) for t in tables]
        + [pl.BlockSpec(w.shape, lambda i, c: (0, 0)) for w in waves]
        + ([grid_block] if carried else [])
    )
    total = sum(t.shape[0] for t in tables)
    return pl.pallas_call(
        functools.partial(inverse_body, len(pieces), block, padded, cols, carried),
        out_shape=jax.ShapeDtypeStruct((rows, cols, longitudes), kind),
        grid_spec=pltpu.PrefetchScalarGridSpec(
            num_scalar_prefetch=1,
            grid=(rows // block,),
            in_specs=in_specs,
            out_specs=grid_block,
            scratch_shapes=[
                pltpu.VMEM((t.shape[0] * padded, cols), jnp.float32) for t in tables
            ],
        ),
        compiler_params=pltpu.CompilerParams(vmem_limit_bytes=VMEM_LIMIT),
        cost_estimate=pl.CostEstimate(
            flops=2 * total * rows * cols * longitudes,
            bytes_accessed=rows * cols * (2 * total + 4 * longitudes),
            transcendentals=0,
        ),
        name="inverse_fourier",
    )(counts, *pieces, *tables, *waves, *([before] if carried else []))


def per_device(lat_size, lev_size, grid, legendre, vertical, damping, lon_counts, wave_slots):
    lat_rows, level_rows, fields, longitudes = grid.shape
    cols = level_rows * fields
    owners = lat_size * lev_size
    rounds = wave_slots.shape[0] // owners
    degrees = legendre.shape[1]
    axes = ("lat", "lev")
    lat, lev = lax.axis_index("lat"), lax.axis_index("lev")
    counts = lax.dynamic_slice_in_dim(lon_counts, lat * lat_rows, lat_rows)
    owner_waves = wave_slots.reshape(owners, rounds)
    own_waves = lax.dynamic_slice_in_dim(wave_slots, (lat * lev_size + lev) * rounds, rounds)

    coupling = lax.all_gather(vertical, "lev", axis=0, tiled=True)
    strength = lax.all_gather(damping, "lev", axis=0, tiled=True)
    mixer = jnp.kron(coupling.T, jnp.eye(fields, dtype=coupling.dtype))
    degree_values = jnp.arange(degrees).astype(jnp.float32)
    ratio = degree_values * (degree_values + 1.0) / float(degrees * (degrees - 1))
    lanes = jnp.repeat(strength.astype(jnp.float32), fields)
    factor = 1.0 / (1.0 + lanes[None, :] * (ratio * ratio)[:, None])

    points = grid.reshape(lat_rows, cols, longitudes)
    chunk_count = min(CHUNKS, rounds)
    edges = [rounds * c // chunk_count for c in range(chunk_count + 1)]
    tables, waves, returned = [], [], []
    for low, high in zip(edges[:-1], edges[1:]):
        count = high - low
        slots = owner_waves[:, low:high].reshape(-1)
        table = table_build(slots, longitudes)
        wave = jnp.broadcast_to(jnp.tile(slots, 2)[:, None], (2 * slots.shape[0], cols))
        fourier = forward_fourier(points, table, wave, counts)
        fourier = fourier.reshape(owners, count, 2, lat_rows, cols)
        gathered = lax.all_to_all(fourier, axes, split_axis=0, concat_axis=0, tiled=True)
        banded = spectral_step(
            legendre,
            gathered,
            mixer,
            factor,
            (lev * rounds + low).reshape(1),
            own_waves[low:high],
            lat_size,
            lev_size,
        )
        back = lax.all_to_all(banded, axes, split_axis=0, concat_axis=0, tiled=True)
        tables.append(table)
        waves.append(wave)
        returned.append(back.reshape(owners * count, 2, lat_rows, cols))
    before = None
    if chunk_count > 1:
        for c in range(chunk_count - 1):
            before = inverse_fourier(
                returned[c : c + 1], tables[c : c + 1], waves[c : c + 1], counts, before, jnp.float32
            )
    filtered = inverse_fourier(
        returned[-1:], tables[-1:], waves[-1:], counts, before, jnp.bfloat16
    )
    return filtered.reshape(lat_rows, level_rows, fields, longitudes)


def solution(mesh):
    return jax.shard_map(
        functools.partial(per_device, mesh.shape["lat"], mesh.shape["lev"]),
        mesh=mesh,
        in_specs=(
            P("lat", "lev", None, None),
            P("lat", None, None),
            P("lev", None),
            P("lev"),
            P(),
            P(),
        ),
        out_specs=P("lat", "lev", None, None),
        check_vma=False,
    )
```
